32 devices in a mesh: data: 1 (over z), model: 4 (over y), stage: 8 (over x, core).
Axes of the slice: x: 4, y: 4, z: 1, core: 2. Of those that a mesh axis runs over, the one named last changes fastest.
The devices are a block of a 4x4x8 slice.
Arguments:
- inputs: bfloat16 [12, 384, 1024], P('data')
- targets: bfloat16 [12, 384, 1024], P('data')
- w_in: bfloat16 [8, 1, 1024, 4096], P('stage', None, None, 'model')
- w_out: bfloat16 [8, 1, 4096, 1024], P('stage', None, 'model')
Outputs:
- output 1: float32 [8, 1, 1024, 4096], P(('data', 'stage'), None, None, 'model')
- output 2: float32 [8, 1, 4096, 1024], P(('data', 'stage'), None, 'model')
- output 3: float32 [1], P('data')
All inputs are finite; a program needn't handle non-finite values.
Results may differ from the reference program's by a relative error of at most 0.00463857.
Values are sent between devices in bfloat16 or wider.
A program may use at most 768 MiB of HBM per device.

```python
import jax
import jax.numpy as jnp
from jax import lax

STAGES = 8
LAYERS_PER_STAGE = 1
MODEL_DIM = 1024
HIDDEN_DIM = 4096
MICRO_BATCHES = 12
MICRO_TOKENS = 384

TOTAL_LAYERS = STAGES * LAYERS_PER_STAGE
GELU_COEF = 0.7978845608028654
CUBIC_COEF = 0.044715


def gelu_tanh(values):
    inner_arg = GELU_COEF * (values + CUBIC_COEF * values * values * values)
    return 0.5 * values * (1.0 + jnp.tanh(inner_arg))


def gelu_slope(values):
    tanh_val = jnp.tanh(GELU_COEF * (values + CUBIC_COEF * values * values * values))
    return 0.5 * (1.0 + tanh_val) + 0.5 * values * (1.0 - tanh_val * tanh_val) * GELU_COEF * (1.0 + 3.0 * CUBIC_COEF * values * values)


def setup_inputs(seed: int = 0, part: int = 0) -> dict:
    part_key = jax.random.fold_in(jax.random.key(seed), part)
    key_in, key_tgt = jax.random.split(part_key, 2)
    key_w1, key_w2 = jax.random.split(jax.random.key(seed + 1), 2)
    act_shape = (MICRO_BATCHES, MICRO_TOKENS, MODEL_DIM)
    inputs = jax.random.normal(key_in, act_shape, jnp.float32).astype(jnp.bfloat16)
    targets = jax.random.normal(key_tgt, act_shape, jnp.float32).astype(jnp.bfloat16)
    in_scale = MODEL_DIM ** -0.5
    out_scale = (HIDDEN_DIM ** -0.5) * (2.0 / TOTAL_LAYERS) ** 0.5
    w_in = (jax.random.normal(key_w1, (STAGES, LAYERS_PER_STAGE, MODEL_DIM, HIDDEN_DIM), jnp.float32) * in_scale).astype(jnp.bfloat16)
    w_out = (jax.random.normal(key_w2, (STAGES, LAYERS_PER_STAGE, HIDDEN_DIM, MODEL_DIM), jnp.float32) * out_scale).astype(jnp.bfloat16)
    return {"inputs": inputs, "targets": targets, "w_in": w_in, "w_out": w_out}


def layer_forward(hidden, w_in_l, w_out_l):
    pre_act = jnp.dot(hidden, w_in_l, preferred_element_type=jnp.float32).astype(jnp.bfloat16)
    act_out = gelu_tanh(pre_act.astype(jnp.float32)).astype(jnp.bfloat16)
    branch = jnp.dot(act_out, w_out_l, preferred_element_type=jnp.float32)
    return (hidden.astype(jnp.float32) + branch).astype(jnp.bfloat16)


def layer_backward(grad_h, hidden, w_in_l, w_out_l):
    pre_act = jnp.dot(hidden, w_in_l, preferred_element_type=jnp.float32).astype(jnp.bfloat16)
    act_out = gelu_tanh(pre_act.astype(jnp.float32)).astype(jnp.bfloat16)
    grad_act = jnp.dot(grad_h, w_out_l.T, preferred_element_type=jnp.float32).astype(jnp.bfloat16)
    grad_pre = (gelu_slope(pre_act.astype(jnp.float32)) * grad_act.astype(jnp.float32)).astype(jnp.bfloat16)
    grad_prev = (grad_h.astype(jnp.float32) + jnp.dot(grad_pre, w_in_l.T, preferred_element_type=jnp.float32)).astype(jnp.bfloat16)
    part_in = jnp.dot(hidden.T, grad_pre, preferred_element_type=jnp.float32)
    part_out = jnp.dot(act_out.T, grad_h, preferred_element_type=jnp.float32)
    return grad_prev, part_in, part_out


def reference(inputs, targets, w_in, w_out):
    w_in_flat = w_in.reshape(TOTAL_LAYERS, MODEL_DIM, HIDDEN_DIM)
    w_out_flat = w_out.reshape(TOTAL_LAYERS, HIDDEN_DIM, MODEL_DIM)
    grad_scale = 1.0 / (MICRO_BATCHES * MICRO_TOKENS * MODEL_DIM)

    def fwd_step(hidden, layer_w):
        return layer_forward(hidden, layer_w[0], layer_w[1]), hidden

    def bwd_step(grad_h, layer_data):
        w_in_l, w_out_l, saved_in, acc_in, acc_out = layer_data
        grad_prev, part_in, part_out = layer_backward(grad_h, saved_in, w_in_l, w_out_l)
        return grad_prev, (acc_in + part_in, acc_out + part_out)

    def micro_step(state_in, micro_pair):
        acc_in, acc_out, loss_sum = state_in
        final_out, saved_in = lax.scan(fwd_step, micro_pair[0], (w_in_flat, w_out_flat))
        out_err = final_out.astype(jnp.float32) - micro_pair[1].astype(jnp.float32)
        start_grad = (out_err * grad_scale).astype(jnp.bfloat16)
        input_grad, (acc_in, acc_out) = lax.scan(bwd_step, start_grad, (w_in_flat, w_out_flat, saved_in, acc_in, acc_out), reverse=True)
        return (acc_in, acc_out, loss_sum + 0.5 * jnp.sum(out_err * out_err)), None

    init_state = (jnp.zeros((TOTAL_LAYERS, MODEL_DIM, HIDDEN_DIM), jnp.float32), jnp.zeros((TOTAL_LAYERS, HIDDEN_DIM, MODEL_DIM), jnp.float32), jnp.zeros((), jnp.float32))
    (acc_in, acc_out, loss_sum), unused_ys = lax.scan(micro_step, init_state, (inputs, targets))
    grad_in = acc_in.reshape(STAGES, LAYERS_PER_STAGE, MODEL_DIM, HIDDEN_DIM)
    grad_out = acc_out.reshape(STAGES, LAYERS_PER_STAGE, HIDDEN_DIM, MODEL_DIM)
    return grad_in, grad_out, jnp.reshape(loss_sum * grad_scale, (1,))
```

```python
import functools

import jax
import jax.numpy as jnp
from jax import lax
from jax.experimental import pallas as pl
from jax.experimental.pallas import tpu as pltpu
from jax.sharding import PartitionSpec as P

GELU_COEF = 0.7978845608028654
CUBIC_COEF = 0.044715
CHUNK = 128
MESH = pl.DeviceIdType.MESH


def gelu_tanh(values):
    inner_arg = GELU_COEF * (values + CUBIC_COEF * values * values * values)
    return 0.5 * values * (1.0 + jnp.tanh(inner_arg))


def gelu_slope(values):
    square = values * values
    tanh_val = jnp.tanh(GELU_COEF * (values + CUBIC_COEF * values * square))
    return 0.5 * (1.0 + tanh_val) + 0.5 * values * (1.0 - tanh_val * tanh_val) * GELU_COEF * (1.0 + 3.0 * CUBIC_COEF * square)


def dot_nn(lhs, rhs):
    return lax.dot_general(lhs, rhs, (((1,), (0,)), ((), ())), preferred_element_type=jnp.float32)


def dot_nt(lhs, rhs):
    return lax.dot_general(lhs, rhs, (((1,), (1,)), ((), ())), preferred_element_type=jnp.float32)


def chain_kernel(
    n_stage, n_model, n_chunk, grad_scale,
    in_hbm, tgt_hbm, w1_hbm, w2_hbm,
    x_all, e_all, loss_out,
    w1_v, w2_v, x_v, e_v, y_v, t_v, u_v, a_v, loss_acc, loss_parts, loss_tot,
    local_sem, w_send, w_recv,
    xp_send, xp_recv, ep_send, ep_recv,
    xg_send, xg_recv, eg_send, eg_recv, gl_sem,
    loss_send, loss_recv,
):
    stage = lax.axis_index("stage")
    me = lax.axis_index("model")
    last = n_stage - 1
    left = lax.rem(me + n_model - 1, n_model)
    right = lax.rem(me + 1, n_model)
    far = lax.rem(me + 2, n_model)
    is_first = stage == 0
    is_last = stage == last
    not_first = stage > 0
    not_last = stage < last
    ring_len = n_chunk
    dim, hid = w1_v.shape[1], w1_v.shape[2]
    half = dim // 2

    def remote(src, dst, send, recv, **where):
        return pltpu.make_async_remote_copy(
            src_ref=src, dst_ref=dst, send_sem=send, recv_sem=recv, device_id=where, device_id_type=MESH
        )

    barrier = pltpu.get_barrier_semaphore()
    for peer in (left, right, far):
        pl.semaphore_signal(barrier, inc=1, device_id={"model": peer}, device_id_type=MESH)

    @pl.when(not_first)
    def _():
        pl.semaphore_signal(barrier, inc=1, device_id={"stage": stage - 1}, device_id_type=MESH)

    @pl.when(not_last)
    def _():
        pl.semaphore_signal(barrier, inc=1, device_id={"stage": stage + 1}, device_id_type=MESH)

    num_peers = 5 - is_first.astype(jnp.int32) - is_last.astype(jnp.int32)
    pl.semaphore_wait(barrier, num_peers)

    def own_piece(w_hbm, w_v, idx, part, peer, slot):
        rows = pl.ds(part * half, half)
        return remote(w_hbm.at[rows], w_v.at[me, rows], w_send.at[idx, slot], w_recv.at[idx, slot], model=peer)

    def passed_piece(w_v, idx, owner, part, peer, slot):
        rows = pl.ds(part * half, half)
        return remote(w_v.at[owner, rows], w_v.at[owner, rows], w_send.at[idx, slot], w_recv.at[idx, slot], model=peer)

    weights = ((w1_hbm, w1_v, 0), (w2_hbm, w2_v, 1))
    def start_own(w_hbm, w_v, idx):
        own_piece(w_hbm, w_v, idx, 0, right, 0).start()
        own_piece(w_hbm, w_v, idx, 1, left, 3).start()
        own_piece(w_hbm, w_v, idx, 1, right, 1).start()
        own_piece(w_hbm, w_v, idx, 0, left, 2).start()

    def pass_on(w_hbm, w_v, idx):
        own_piece(w_hbm, w_v, idx, 0, right, 0).wait_recv()
        passed_piece(w_v, idx, left, 0, right, 4).start()
        own_piece(w_hbm, w_v, idx, 1, left, 3).wait_recv()
        passed_piece(w_v, idx, right, 1, left, 5).start()

    def finish_recv(w_hbm, w_v, idx):
        own_piece(w_hbm, w_v, idx, 1, right, 1).wait_recv()
        own_piece(w_hbm, w_v, idx, 0, left, 2).wait_recv()
        passed_piece(w_v, idx, left, 0, right, 4).wait_recv()
        passed_piece(w_v, idx, right, 1, left, 5).wait_recv()

    def finish_send(w_hbm, w_v, idx):
        own_piece(w_hbm, w_v, idx, 0, right, 0).wait_send()
        own_piece(w_hbm, w_v, idx, 1, left, 3).wait_send()
        own_piece(w_hbm, w_v, idx, 1, right, 1).wait_send()
        own_piece(w_hbm, w_v, idx, 0, left, 2).wait_send()
        passed_piece(w_v, idx, left, 0, right, 4).wait_send()
        passed_piece(w_v, idx, right, 1, left, 5).wait_send()

    start_own(*weights[0])
    own_copies = [pltpu.make_async_copy(w_hbm, w_v.at[me], local_sem.at[idx]) for w_hbm, w_v, idx in weights]
    for copy in own_copies:
        copy.start()
    mine = pl.ds(me * n_chunk, n_chunk)

    @pl.when(is_first)
    def _():
        load = pltpu.make_async_copy(in_hbm.at[mine], x_v, local_sem.at[2])
        load.start()
        load.wait()
        store = pltpu.make_async_copy(x_v, x_all.at[mine], local_sem.at[2])
        store.start()
        store.wait()
        for owner in (left, right, far):
            block = pl.ds(owner * n_chunk, n_chunk)
            load = pltpu.make_async_copy(in_hbm.at[block], t_v, local_sem.at[2])
            load.start()
            load.wait()
            store = pltpu.make_async_copy(t_v, x_all.at[block], local_sem.at[2])
            store.start()
            store.wait()

    @pl.when(is_last)
    def _():
        load = pltpu.make_async_copy(tgt_hbm.at[mine], t_v, local_sem.at[2])
        load.start()
        load.wait()
        loss_acc[...] = jnp.zeros_like(loss_acc)

    pass_on(*weights[0])
    start_own(*weights[1])
    pass_on(*weights[1])
    for copy in own_copies:
        copy.wait()
    finish_recv(*weights[0])
    finish_recv(*weights[1])

    def shared(src_v, dst_all, send, recv, pos, to_right):
        kind, peer = (0, right) if to_right else (1, left)
        return remote(src_v.at[pos], dst_all.at[me * n_chunk + pos], send.at[kind, pos], recv.at[kind, pos], model=peer)

    def passed(dst_all, send, recv, pos, to_right):
        owner, peer = (left, right) if to_right else (right, left)
        row = owner * n_chunk + pos
        return remote(dst_all.at[row], dst_all.at[row], send.at[2, pos], recv.at[2, pos], model=peer)

    def own_store(src_v, dst_all, idx, pos):
        return pltpu.make_async_copy(src_v.at[pos], dst_all.at[me * n_chunk + pos], gl_sem.at[idx, pos])

    def start_shared(src_v, dst_all, send, recv, idx, pos):
        shared(src_v, dst_all, send, recv, pos, True).start()
        shared(src_v, dst_all, send, recv, pos, False).start()
        own_store(src_v, dst_all, idx, pos).start()

    def relay(src_v, dst_all, send, recv, pos):
        @pl.when(lax.rem(pos, 2) == 0)
        def _():
            shared(src_v, dst_all, send, recv, pos, True).wait_recv()
            passed(dst_all, send, recv, pos, True).start()

        @pl.when(lax.rem(pos, 2) == 1)
        def _():
            shared(src_v, dst_all, send, recv, pos, False).wait_recv()
            passed(dst_all, send, recv, pos, False).start()

    def finish_gather(src_v, dst_all, send, recv, idx, pos):
        shared(src_v, dst_all, send, recv, pos, True).wait_send()
        shared(src_v, dst_all, send, recv, pos, False).wait_send()
        own_store(src_v, dst_all, idx, pos).wait()

        @pl.when(lax.rem(pos, 2) == 0)
        def _():
            shared(src_v, dst_all, send, recv, pos, False).wait_recv()
            passed(dst_all, send, recv, pos, True).wait()

        @pl.when(lax.rem(pos, 2) == 1)
        def _():
            shared(src_v, dst_all, send, recv, pos, True).wait_recv()
            passed(dst_all, send, recv, pos, False).wait()

    x_gather = (x_v, x_all, xg_send, xg_recv)
    e_gather = (e_v, e_all, eg_send, eg_recv)

    def act_copy(pos):
        return remote(y_v.at[pos], x_v.at[pos], xp_send.at[pos], xp_recv.at[pos], stage=stage + 1)

    def grad_copy(pos):
        return remote(y_v.at[pos], e_v.at[pos], ep_send.at[pos], ep_recv.at[pos], stage=stage - 1)

    @pl.loop(0, n_chunk)
    def _(pos):
        @pl.when(not_first)
        def _():
            act_copy(pos).wait_recv()
            start_shared(*x_gather, 0, pos)

        for part in range(n_model):
            cols = pl.ds(part * hid, hid)
            pre = dot_nn(x_v[pos], w1_v[part]).astype(jnp.bfloat16)
            u_v[pos, :, cols] = pre
            a_v[:, cols] = gelu_tanh(pre.astype(jnp.float32)).astype(jnp.bfloat16)
        branch = dot_nn(a_v[...], w2_v[...].reshape(n_model * hid, dim))
        y_v[pos] = (x_v[pos].astype(jnp.float32) + branch).astype(jnp.bfloat16)

        @pl.when(not_last)
        def _():
            act_copy(pos).start()

        @pl.when(is_last)
        def _():
            err = y_v[pos].astype(jnp.float32) - t_v[pos].astype(jnp.float32)
            e_v[pos] = (err * grad_scale).astype(jnp.bfloat16)
            loss_acc[...] += jnp.sum((err * err).reshape(-1, 8, dim), axis=0)

    def loss_share(kind, peer):
        return remote(loss_parts.at[0], loss_parts.at[1 + kind], loss_send.at[kind], loss_recv.at[kind], model=peer)

    @pl.when(is_last)
    def _():
        loss_parts[0] = jnp.full((8, 128), 0.5 * jnp.sum(loss_acc[...]), jnp.float32)

    @pl.loop(0, n_chunk)
    def _(pos):
        @pl.when(not_last)
        def _():
            grad_copy(pos).wait_recv()

        start_shared(*e_gather, 1, pos)

        @pl.when(not_last)
        def _():
            act_copy(pos).wait_send()

        @pl.when(not_first)
        def _():
            relay(*x_gather, pos)
            for part in range(n_model):
                cols = pl.ds(part * hid, hid)
                grad_act = dot_nt(e_v[pos], w2_v[part]).astype(jnp.bfloat16)
                slope = gelu_slope(u_v[pos, :, cols].astype(jnp.float32))
                a_v[:, cols] = (slope * grad_act.astype(jnp.float32)).astype(jnp.bfloat16)
            total = e_v[pos].astype(jnp.float32)
            branch = dot_nt(a_v[:, pl.ds(0, hid)], w1_v[0])
            for part in range(1, n_model):
                branch += dot_nt(a_v[:, pl.ds(part * hid, hid)], w1_v[part])
            y_v[pos] = (total + branch).astype(jnp.bfloat16)
            grad_copy(pos).start()

    def loss_down():
        return remote(loss_tot, loss_tot, loss_send.at[3], loss_recv.at[3], stage=stage - 1)

    @pl.when(is_last)
    def _():
        shares = [loss_share(kind, peer) for kind, peer in enumerate((left, right, far))]
        for copy in shares:
            copy.start()
        for copy in shares:
            copy.wait()
        pair_sum = (loss_parts[0] + loss_parts[3]) + (loss_parts[1] + loss_parts[2])
        loss_tot[...] = pair_sum * grad_scale

    @pl.when(not_last)
    def _():
        loss_down().wait_recv()

    @pl.when(not_first)
    def _():
        loss_down().start()

    for weight in weights:
        finish_send(*weight)

    @pl.loop(0, n_chunk)
    def _(pos):
        relay(*e_gather, pos)

    @pl.loop(0, n_chunk)
    def _(pos):
        @pl.when(not_first)
        def _():
            grad_copy(pos).wait_send()
            finish_gather(*x_gather, 0, pos)

        finish_gather(*e_gather, 1, pos)

    @pl.when(not_first)
    def _():
        loss_down().wait_send()

    loss_out[...] = loss_tot[...]


def solution(mesh):
    n_stage = mesh.shape["stage"]
    n_model = mesh.shape["model"]

    def stage_step(inputs, targets, w_in, w_out):
        num_micro, num_tokens, dim = inputs.shape
        hid = w_in.shape[3]
        w1, w2 = w_in[0, 0], w_out[0, 0]
        tokens = num_micro * num_tokens
        grad_scale = 1.0 / (tokens * dim)
        n_chunk = tokens // (n_model * CHUNK)
        chunked = (n_model * n_chunk, CHUNK, dim)
        any_spec = pl.BlockSpec(memory_space=pl.ANY)
        dma = pltpu.SemaphoreType.DMA
        block = pltpu.VMEM((n_chunk, CHUNK, dim), jnp.bfloat16)
        x_all, e_all, loss = pl.pallas_call(
            functools.partial(chain_kernel, n_stage, n_model, n_chunk, grad_scale),
            out_shape=(
                jax.ShapeDtypeStruct(chunked, jnp.bfloat16),
                jax.ShapeDtypeStruct(chunked, jnp.bfloat16),
                jax.ShapeDtypeStruct((8, 128), jnp.float32),
            ),
            in_specs=[any_spec] * 4,
            out_specs=(any_spec, any_spec, pl.BlockSpec(memory_space=pltpu.VMEM)),
            scratch_shapes=[
                pltpu.VMEM((n_model, dim, hid), jnp.bfloat16),
                pltpu.VMEM((n_model, hid, dim), jnp.bfloat16),
                block, block, block, block,
                pltpu.VMEM((n_chunk, CHUNK, n_model * hid), jnp.bfloat16),
                pltpu.VMEM((CHUNK, n_model * hid), jnp.bfloat16),
                pltpu.VMEM((8, dim), jnp.float32),
                pltpu.VMEM((4, 8, 128), jnp.float32),
                pltpu.VMEM((8, 128), jnp.float32),
                dma((3,)), dma((2, 6)), dma((2, 6)),
                dma((n_chunk,)), dma((n_chunk,)), dma((n_chunk,)), dma((n_chunk,)),
                dma((3, n_chunk)), dma((3, n_chunk)), dma((3, n_chunk)), dma((3, n_chunk)), dma((2, n_chunk)),
                dma((4,)), dma((4,)),
            ],
            compiler_params=pltpu.CompilerParams(
                collective_id=0, has_side_effects=True, vmem_limit_bytes=60 * 1024 * 1024
            ),
        )(inputs.reshape(chunked), targets.reshape(chunked), w1, w2)
        x_full = x_all.reshape(tokens, dim)
        e_full = e_all.reshape(tokens, dim)
        pre = dot_nn(x_full, w1).astype(jnp.bfloat16)
        act = gelu_tanh(pre.astype(jnp.float32)).astype(jnp.bfloat16)
        grad_act = dot_nt(e_full, w2).astype(jnp.bfloat16)
        grad_pre = (gelu_slope(pre.astype(jnp.float32)) * grad_act.astype(jnp.float32)).astype(jnp.bfloat16)
        contract_rows = (((0,), (0,)), ((), ()))
        grad_out = lax.dot_general(act, e_full, contract_rows, preferred_element_type=jnp.float32)
        grad_in = lax.dot_general(x_full, grad_pre, contract_rows, preferred_element_type=jnp.float32)
        return grad_in[None, None], grad_out[None, None], loss[0, :1]

    return jax.shard_map(
        stage_step,
        mesh=mesh,
        in_specs=(P("data", None, None), P("data", None, None), P("stage", None, None, "model"), P("stage", None, "model", None)),
        out_specs=(P(("data", "stage"), None, None, "model"), P(("data", "stage"), None, "model", None), P("data")),
        check_vma=False,
    )
```

```python
import functools

import jax
import jax.numpy as jnp
from jax import lax
from jax.experimental import pallas as pl
from jax.experimental.pallas import tpu as pltpu
from jax.sharding import PartitionSpec as P

GELU_COEF = 0.7978845608028654
CUBIC_COEF = 0.044715
CHUNK = 128
MESH = pl.DeviceIdType.MESH


def gelu_tanh(values):
    inner_arg = GELU_COEF * (values + CUBIC_COEF * values * values * values)
    return 0.5 * values * (1.0 + jnp.tanh(inner_arg))


def gelu_slope(values):
    square = values * values
    tanh_val = jnp.tanh(GELU_COEF * (values + CUBIC_COEF * values * square))
    return 0.5 * (1.0 + tanh_val) + 0.5 * values * (1.0 - tanh_val * tanh_val) * GELU_COEF * (1.0 + 3.0 * CUBIC_COEF * square)


def dot_nn(lhs, rhs):
    return lax.dot_general(lhs, rhs, (((1,), (0,)), ((), ())), preferred_element_type=jnp.float32)


def dot_nt(lhs, rhs):
    return lax.dot_general(lhs, rhs, (((1,), (1,)), ((), ())), preferred_element_type=jnp.float32)


def dot_tn(lhs, rhs):
    return lax.dot_general(lhs, rhs, (((0,), (0,)), ((), ())), preferred_element_type=jnp.float32)


def step_kernel(
    n_stage, n_model, n_chunk, grad_scale,
    in_hbm, tgt_hbm, w1_hbm, w2_hbm,
    dw1, dw2, loss_out,
    w1_v, w2_v, x_v, e_v, yf_v, yb_v, u_v, a_v, du_v, da_v, loss_acc, loss_parts, loss_tot,
    local_sem, w_send, w_recv,
    xp_send, xp_recv, ep_send, ep_recv,
    xg_send, xg_recv, eg_send, eg_recv,
    loss_send, loss_recv,
):
    stage = lax.axis_index("stage")
    me = lax.axis_index("model")
    last = n_stage - 1
    left = lax.rem(me + n_model - 1, n_model)
    right = lax.rem(me + 1, n_model)
    far = lax.rem(me + 2, n_model)
    is_first = stage == 0
    is_last = stage == last
    not_first = stage > 0
    not_last = stage < last
    dim, hid = w1_v.shape[1], w1_v.shape[2]
    half = dim // 2
    rows_all = n_model * CHUNK

    def remote(src, dst, send, recv, **where):
        return pltpu.make_async_remote_copy(
            src_ref=src, dst_ref=dst, send_sem=send, recv_sem=recv, device_id=where, device_id_type=MESH
        )

    barrier = pltpu.get_barrier_semaphore()
    for peer in (left, right, far):
        pl.semaphore_signal(barrier, inc=1, device_id={"model": peer}, device_id_type=MESH)

    @pl.when(not_first)
    def _():
        pl.semaphore_signal(barrier, inc=1, device_id={"stage": stage - 1}, device_id_type=MESH)

    @pl.when(not_last)
    def _():
        pl.semaphore_signal(barrier, inc=1, device_id={"stage": stage + 1}, device_id_type=MESH)

    num_peers = 5 - is_first.astype(jnp.int32) - is_last.astype(jnp.int32)
    pl.semaphore_wait(barrier, num_peers)

    def own_piece(w_hbm, w_v, idx, part, peer, slot):
        rows = pl.ds(part * half, half)
        return remote(w_hbm.at[rows], w_v.at[me, rows], w_send.at[idx, slot], w_recv.at[idx, slot], model=peer)

    def passed_piece(w_v, idx, owner, part, peer, slot):
        rows = pl.ds(part * half, half)
        return remote(w_v.at[owner, rows], w_v.at[owner, rows], w_send.at[idx, slot], w_recv.at[idx, slot], model=peer)

    weights = ((w1_hbm, w1_v, 0), (w2_hbm, w2_v, 1))
    def start_own(w_hbm, w_v, idx):
        own_piece(w_hbm, w_v, idx, 0, right, 0).start()
        own_piece(w_hbm, w_v, idx, 1, left, 3).start()
        own_piece(w_hbm, w_v, idx, 1, right, 1).start()
        own_piece(w_hbm, w_v, idx, 0, left, 2).start()

    def pass_on(w_hbm, w_v, idx):
        own_piece(w_hbm, w_v, idx, 0, right, 0).wait_recv()
        passed_piece(w_v, idx, left, 0, right, 4).start()
        own_piece(w_hbm, w_v, idx, 1, left, 3).wait_recv()
        passed_piece(w_v, idx, right, 1, left, 5).start()

    def finish_recv(w_hbm, w_v, idx):
        own_piece(w_hbm, w_v, idx, 1, right, 1).wait_recv()
        own_piece(w_hbm, w_v, idx, 0, left, 2).wait_recv()
        passed_piece(w_v, idx, left, 0, right, 4).wait_recv()
        passed_piece(w_v, idx, right, 1, left, 5).wait_recv()

    def finish_send(w_hbm, w_v, idx):
        own_piece(w_hbm, w_v, idx, 0, right, 0).wait_send()
        own_piece(w_hbm, w_v, idx, 1, left, 3).wait_send()
        own_piece(w_hbm, w_v, idx, 1, right, 1).wait_send()
        own_piece(w_hbm, w_v, idx, 0, left, 2).wait_send()
        passed_piece(w_v, idx, left, 0, right, 4).wait_send()
        passed_piece(w_v, idx, right, 1, left, 5).wait_send()

    start_own(*weights[0])
    own_copies = [pltpu.make_async_copy(w_hbm, w_v.at[me], local_sem.at[idx]) for w_hbm, w_v, idx in weights]
    for copy in own_copies:
        copy.start()

    @pl.when(is_first)
    def _():
        loads = [pltpu.make_async_copy(in_hbm.at[owner], x_v.at[:, owner], local_sem.at[2 + owner]) for owner in range(n_model)]
        for load in loads:
            load.start()
        for load in loads:
            load.wait()

    @pl.when(is_last)
    def _():
        load = pltpu.make_async_copy(tgt_hbm.at[me], e_v.at[:, me], local_sem.at[2])
        load.start()
        load.wait()
        loss_acc[...] = jnp.zeros_like(loss_acc)

    dw1[...] = jnp.zeros_like(dw1)
    dw2[...] = jnp.zeros_like(dw2)

    pass_on(*weights[0])
    start_own(*weights[1])
    pass_on(*weights[1])
    for copy in own_copies:
        copy.wait()
    finish_recv(*weights[0])
    finish_recv(*weights[1])

    def shared(buf, send, recv, pos, to_right):
        kind, peer = (0, right) if to_right else (1, left)
        return remote(buf.at[pos, me], buf.at[pos, me], send.at[kind, pos], recv.at[kind, pos], model=peer)

    def passed(buf, send, recv, pos, to_right):
        owner, peer = (left, right) if to_right else (right, left)
        return remote(buf.at[pos, owner], buf.at[pos, owner], send.at[2, pos], recv.at[2, pos], model=peer)

    def start_shared(gather, pos):
        shared(*gather, pos, True).start()
        shared(*gather, pos, False).start()

    def by_parity(pos, even_fn, odd_fn):
        pl.when(lax.rem(pos, 2) == 0)(even_fn)
        pl.when(lax.rem(pos, 2) == 1)(odd_fn)

    def relay(gather, pos):
        def go(to_right):
            shared(*gather, pos, to_right).wait_recv()
            passed(*gather, pos, to_right).start()

        by_parity(pos, lambda: go(True), lambda: go(False))

    def arrived(gather, pos):
        def go(to_right):
            shared(*gather, pos, not to_right).wait_recv()
            passed(*gather, pos, to_right).wait_recv()

        by_parity(pos, lambda: go(True), lambda: go(False))

    def finish_gather(gather, pos):
        shared(*gather, pos, True).wait_send()
        shared(*gather, pos, False).wait_send()
        by_parity(pos, lambda: passed(*gather, pos, True).wait_send(), lambda: passed(*gather, pos, False).wait_send())

    x_gather = (x_v, xg_send, xg_recv)
    e_gather = (e_v, eg_send, eg_recv)

    def act_copy(pos):
        return remote(yf_v.at[lax.rem(pos, 2)], x_v.at[pos, me], xp_send.at[pos], xp_recv.at[pos], stage=stage + 1)

    def grad_copy(pos):
        return remote(yb_v.at[lax.rem(pos, 2)], e_v.at[pos, me], ep_send.at[pos], ep_recv.at[pos], stage=stage - 1)

    def forward(pos):
        @pl.when(not_first)
        def _():
            act_copy(pos).wait_recv()
            start_shared(x_gather, pos)

        @pl.when(not_last & (pos >= 2))
        def _():
            act_copy(pos - 2).wait_send()

        slot = lax.rem(pos, 2)
        for part in range(n_model):
            cols = pl.ds(part * hid, hid)
            pre = dot_nn(x_v[pos, me], w1_v[part]).astype(jnp.bfloat16)
            u_v[pos, :, cols] = pre
            a_v[:, cols] = gelu_tanh(pre.astype(jnp.float32)).astype(jnp.bfloat16)
        branch = dot_nn(a_v[...], w2_v[...].reshape(n_model * hid, dim))
        yf_v[slot] = (x_v[pos, me].astype(jnp.float32) + branch).astype(jnp.bfloat16)

        @pl.when(not_last)
        def _():
            act_copy(pos).start()

        @pl.when(is_last)
        def _():
            err = yf_v[slot].astype(jnp.float32) - e_v[pos, me].astype(jnp.float32)
            e_v[pos, me] = (err * grad_scale).astype(jnp.bfloat16)
            loss_acc[...] += jnp.sum((err * err).reshape(-1, 8, dim), axis=0)

    def backward(pos):
        @pl.when(not_last)
        def _():
            grad_copy(pos).wait_recv()

        start_shared(e_gather, pos)

        @pl.when(not_first)
        def _():
            @pl.when(pos >= 2)
            def _():
                grad_copy(pos - 2).wait_send()

            for part in range(n_model):
                cols = pl.ds(part * hid, hid)
                grad_act = dot_nt(e_v[pos, me], w2_v[part]).astype(jnp.bfloat16)
                slope = gelu_slope(u_v[pos, :, cols].astype(jnp.float32))
                a_v[:, cols] = (slope * grad_act.astype(jnp.float32)).astype(jnp.bfloat16)
            branch = dot_nt(a_v[:, pl.ds(0, hid)], w1_v[0])
            for part in range(1, n_model):
                branch += dot_nt(a_v[:, pl.ds(part * hid, hid)], w1_v[part])
            yb_v[lax.rem(pos, 2)] = (e_v[pos, me].astype(jnp.float32) + branch).astype(jnp.bfloat16)
            grad_copy(pos).start()

    def weight_grads(pos):
        @pl.when(not_first)
        def _():
            arrived(x_gather, pos)

        arrived(e_gather, pos)
        pre = dot_nn(x_v[pos].reshape(rows_all, dim), w1_v[me]).astype(jnp.bfloat16)
        du_v[...] = pre
        da_v[...] = gelu_tanh(pre.astype(jnp.float32)).astype(jnp.bfloat16)
        dw2[...] += dot_tn(da_v[...], e_v[pos].reshape(rows_all, dim))
        grad_act = dot_nt(e_v[pos].reshape(rows_all, dim), w2_v[me]).astype(jnp.bfloat16)
        slope = gelu_slope(du_v[...].astype(jnp.float32))
        da_v[...] = (slope * grad_act.astype(jnp.float32)).astype(jnp.bfloat16)
        dw1[...] += dot_tn(x_v[pos].reshape(rows_all, dim), da_v[...])

    def loss_share(kind, peer):
        return remote(loss_parts.at[0], loss_parts.at[1 + kind], loss_send.at[kind], loss_recv.at[kind], model=peer)

    def loss_down():
        return remote(loss_tot, loss_tot, loss_send.at[3], loss_recv.at[3], stage=stage - 1)

    warm = jnp.minimum(n_chunk, 1 + 3 * (last - stage)) - 1
    is_late = stage >= n_stage // 2
    relay_at = jnp.where(is_late, warm + n_chunk - 2, warm + 1)
    grads_at = jnp.where(is_late, warm + n_chunk, warm + 2)
    loss_at = jnp.where(is_late, grads_at, grads_at + n_chunk - 2)
    x_lag = 5

    def due(turn, start, fn):
        pos = turn - start
        pl.when((pos >= 0) & (pos < n_chunk))(lambda: fn(pos))

    @pl.loop(0, grads_at + n_chunk)
    def _(turn):
        due(turn, 0, forward)
        due(turn, warm, backward)

        @pl.when(not_first)
        def _():
            due(turn, x_lag, functools.partial(relay, x_gather))

        due(turn, relay_at, functools.partial(relay, e_gather))

        @pl.when(is_last & (turn == n_chunk - 1))
        def _():
            loss_parts[0] = jnp.full((8, 128), 0.5 * jnp.sum(loss_acc[...]), jnp.float32)

        @pl.when(turn == loss_at)
        def _():
            @pl.when(is_last)
            def _():
                shares = [loss_share(kind, peer) for kind, peer in enumerate((left, right, far))]
                for copy in shares:
                    copy.start()
                for copy in shares:
                    copy.wait()
                pair_sum = (loss_parts[0] + loss_parts[3]) + (loss_parts[1] + loss_parts[2])
                loss_tot[...] = pair_sum * grad_scale

            @pl.when(not_last)
            def _():
                loss_down().wait_recv()

            @pl.when(not_first)
            def _():
                loss_down().start()

        due(turn, grads_at, weight_grads)

    for weight in weights:
        finish_send(*weight)

    @pl.loop(0, n_chunk)
    def _(pos):
        @pl.when(not_first)
        def _():
            finish_gather(x_gather, pos)

        finish_gather(e_gather, pos)

    for pos in (n_chunk - 2, n_chunk - 1):
        @pl.when(not_last)
        def _():
            act_copy(pos).wait_send()

        @pl.when(not_first)
        def _():
            grad_copy(pos).wait_send()

    @pl.when(not_first)
    def _():
        loss_down().wait_send()

    loss_out[...] = loss_tot[...]


def solution(mesh):
    n_stage = mesh.shape["stage"]
    n_model = mesh.shape["model"]

    def stage_step(inputs, targets, w_in, w_out):
        num_micro, num_tokens, dim = inputs.shape
        hid = w_in.shape[3]
        w1, w2 = w_in[0, 0], w_out[0, 0]
        tokens = num_micro * num_tokens
        grad_scale = 1.0 / (tokens * dim)
        n_chunk = tokens // (n_model * CHUNK)
        by_owner = (n_model, n_chunk, CHUNK, dim)
        any_spec = pl.BlockSpec(memory_space=pl.ANY)
        vmem_spec = pl.BlockSpec(memory_space=pltpu.VMEM)
        dma = pltpu.SemaphoreType.DMA
        bf16, f32 = jnp.bfloat16, jnp.float32
        dw1, dw2, loss = pl.pallas_call(
            functools.partial(step_kernel, n_stage, n_model, n_chunk, grad_scale),
            out_shape=(
                jax.ShapeDtypeStruct((dim, hid), f32),
                jax.ShapeDtypeStruct((hid, dim), f32),
                jax.ShapeDtypeStruct((8, 128), f32),
            ),
            in_specs=[any_spec] * 4,
            out_specs=(vmem_spec, vmem_spec, vmem_spec),
            scratch_shapes=[
                pltpu.VMEM((n_model, dim, hid), bf16),
                pltpu.VMEM((n_model, hid, dim), bf16),
                pltpu.VMEM((n_chunk, n_model, CHUNK, dim), bf16),
                pltpu.VMEM((n_chunk, n_model, CHUNK, dim), bf16),
                pltpu.VMEM((2, CHUNK, dim), bf16),
                pltpu.VMEM((2, CHUNK, dim), bf16),
                pltpu.VMEM((n_chunk, CHUNK, n_model * hid), bf16),
                pltpu.VMEM((CHUNK, n_model * hid), bf16),
                pltpu.VMEM((n_model * CHUNK, hid), bf16),
                pltpu.VMEM((n_model * CHUNK, hid), bf16),
                pltpu.VMEM((8, dim), f32),
                pltpu.VMEM((4, 8, 128), f32),
                pltpu.VMEM((8, 128), f32),
                dma((2 + n_model,)), dma((2, 6)), dma((2, 6)),
                dma((n_chunk,)), dma((n_chunk,)), dma((n_chunk,)), dma((n_chunk,)),
                dma((3, n_chunk)), dma((3, n_chunk)), dma((3, n_chunk)), dma((3, n_chunk)),
                dma((4,)), dma((4,)),
            ],
            compiler_params=pltpu.CompilerParams(
                collective_id=0, has_side_effects=True, vmem_limit_bytes=67043328
            ),
        )(inputs.reshape(by_owner), targets.reshape(by_owner), w1, w2)
        return dw1[None, None], dw2[None, None], loss[0, :1]

    return jax.shard_map(
        stage_step,
        mesh=mesh,
        in_specs=(P("data", None, None), P("data", None, None), P("stage", None, None, "model"), P("stage", None, "model", None)),
        out_specs=(P(("data", "stage"), None, None, "model"), P(("data", "stage"), None, "model", None), P("data")),
        check_vma=False,
    )
```

```python
import functools

import jax
import jax.numpy as jnp
from jax import lax
from jax.experimental import pallas as pl
from jax.experimental.pallas import tpu as pltpu
from jax.sharding import PartitionSpec as P

GELU_COEF = 0.7978845608028654
CUBIC_COEF = 0.044715
CHUNK = 128
MESH = pl.DeviceIdType.MESH


def gelu_tanh(values):
    inner_arg = GELU_COEF * (values + CUBIC_COEF * values * values * values)
    return 0.5 * values * (1.0 + jnp.tanh(inner_arg))


def gelu_slope(values):
    square = values * values
    tanh_val = jnp.tanh(GELU_COEF * (values + CUBIC_COEF * values * square))
    return 0.5 * (1.0 + tanh_val) + 0.5 * values * (1.0 - tanh_val * tanh_val) * GELU_COEF * (1.0 + 3.0 * CUBIC_COEF * square)


def dot_nn(lhs, rhs):
    return lax.dot_general(lhs, rhs, (((1,), (0,)), ((), ())), preferred_element_type=jnp.float32)


def dot_nt(lhs, rhs):
    return lax.dot_general(lhs, rhs, (((1,), (1,)), ((), ())), preferred_element_type=jnp.float32)


def dot_tn(lhs, rhs):
    return lax.dot_general(lhs, rhs, (((0,), (0,)), ((), ())), preferred_element_type=jnp.float32)


def step_kernel(
    n_stage, n_model, n_chunk, grad_scale,
    in_hbm, tgt_hbm, w1_hbm, w2_hbm,
    dw1, dw2, loss_out,
    w1_v, w2_v, x_v, e_v, yf_v, yb_v, u_v, a_v, du_v, da_v, loss_acc, loss_parts, loss_tot,
    local_sem, w_send, w_recv,
    xp_send, xp_recv, ep_send, ep_recv,
    xg_send, xg_recv, eg_send, eg_recv,
    loss_send, loss_recv,
):
    stage = lax.axis_index("stage")
    me = lax.axis_index("model")
    last = n_stage - 1
    left = lax.rem(me + n_model - 1, n_model)
    right = lax.rem(me + 1, n_model)
    far = lax.rem(me + 2, n_model)
    is_first = stage == 0
    is_last = stage == last
    not_first = stage > 0
    not_last = stage < last
    dim, hid = w1_v.shape[1], w1_v.shape[2]
    half = dim // 2
    rows_all = n_model * CHUNK

    def remote(src, dst, send, recv, **where):
        return pltpu.make_async_remote_copy(
            src_ref=src, dst_ref=dst, send_sem=send, recv_sem=recv, device_id=where, device_id_type=MESH
        )

    barrier = pltpu.get_barrier_semaphore()
    for peer in (left, right, far):
        pl.semaphore_signal(barrier, inc=1, device_id={"model": peer}, device_id_type=MESH)

    @pl.when(not_first)
    def _():
        pl.semaphore_signal(barrier, inc=1, device_id={"stage": stage - 1}, device_id_type=MESH)

    @pl.when(not_last)
    def _():
        pl.semaphore_signal(barrier, inc=1, device_id={"stage": stage + 1}, device_id_type=MESH)

    num_peers = 5 - is_first.astype(jnp.int32) - is_last.astype(jnp.int32)
    pl.semaphore_wait(barrier, num_peers)

    def own_piece(w_hbm, w_v, idx, part, peer, slot):
        rows = pl.ds(part * half, half)
        return remote(w_hbm.at[rows], w_v.at[me, rows], w_send.at[idx, slot], w_recv.at[idx, slot], model=peer)

    def passed_piece(w_v, idx, owner, part, peer, slot):
        rows = pl.ds(part * half, half)
        return remote(w_v.at[owner, rows], w_v.at[owner, rows], w_send.at[idx, slot], w_recv.at[idx, slot], model=peer)

    weights = ((w1_hbm, w1_v, 0), (w2_hbm, w2_v, 1))
    def start_own(w_hbm, w_v, idx):
        own_piece(w_hbm, w_v, idx, 0, right, 0).start()
        own_piece(w_hbm, w_v, idx, 1, left, 3).start()
        own_piece(w_hbm, w_v, idx, 1, right, 1).start()
        own_piece(w_hbm, w_v, idx, 0, left, 2).start()

    def pass_on(w_hbm, w_v, idx):
        own_piece(w_hbm, w_v, idx, 0, right, 0).wait_recv()
        passed_piece(w_v, idx, left, 0, right, 4).start()
        own_piece(w_hbm, w_v, idx, 1, left, 3).wait_recv()
        passed_piece(w_v, idx, right, 1, left, 5).start()

    def finish_recv(w_hbm, w_v, idx):
        own_piece(w_hbm, w_v, idx, 1, right, 1).wait_recv()
        own_piece(w_hbm, w_v, idx, 0, left, 2).wait_recv()
        passed_piece(w_v, idx, left, 0, right, 4).wait_recv()
        passed_piece(w_v, idx, right, 1, left, 5).wait_recv()

    def finish_send(w_hbm, w_v, idx):
        own_piece(w_hbm, w_v, idx, 0, right, 0).wait_send()
        own_piece(w_hbm, w_v, idx, 1, left, 3).wait_send()
        own_piece(w_hbm, w_v, idx, 1, right, 1).wait_send()
        own_piece(w_hbm, w_v, idx, 0, left, 2).wait_send()
        passed_piece(w_v, idx, left, 0, right, 4).wait_send()
        passed_piece(w_v, idx, right, 1, left, 5).wait_send()

    start_own(*weights[0])
    own_copies = [pltpu.make_async_copy(w_hbm, w_v.at[me], local_sem.at[idx]) for w_hbm, w_v, idx in weights]
    for copy in own_copies:
        copy.start()

    @pl.when(is_first)
    def _():
        loads = [pltpu.make_async_copy(in_hbm.at[owner], x_v.at[:, owner], local_sem.at[2 + owner]) for owner in range(n_model)]
        for load in loads:
            load.start()
        for load in loads:
            load.wait()

    @pl.when(is_last)
    def _():
        load = pltpu.make_async_copy(tgt_hbm.at[me], e_v.at[:, me], local_sem.at[2])
        load.start()
        load.wait()
        loss_acc[...] = jnp.zeros_like(loss_acc)

    dw1[...] = jnp.zeros_like(dw1)
    dw2[...] = jnp.zeros_like(dw2)

    pass_on(*weights[0])
    start_own(*weights[1])
    pass_on(*weights[1])
    for copy in own_copies:
        copy.wait()
    finish_recv(*weights[0])
    finish_recv(*weights[1])

    def shared(buf, send, recv, pos, to_right):
        kind, peer = (0, right) if to_right else (1, left)
        return remote(buf.at[pos, me], buf.at[pos, me], send.at[kind, pos], recv.at[kind, pos], model=peer)

    def passed(buf, send, recv, pos, to_right):
        owner, peer = (left, right) if to_right else (right, left)
        return remote(buf.at[pos, owner], buf.at[pos, owner], send.at[2, pos], recv.at[2, pos], model=peer)

    def start_shared(gather, pos):
        shared(*gather, pos, True).start()
        shared(*gather, pos, False).start()

    def by_parity(pos, even_fn, odd_fn):
        pl.when(lax.rem(pos, 2) == 0)(even_fn)
        pl.when(lax.rem(pos, 2) == 1)(odd_fn)

    def relay(gather, pos):
        def go(to_right):
            shared(*gather, pos, to_right).wait_recv()
            passed(*gather, pos, to_right).start()

        by_parity(pos, lambda: go(True), lambda: go(False))

    def arrived(gather, pos):
        def go(to_right):
            shared(*gather, pos, not to_right).wait_recv()
            passed(*gather, pos, to_right).wait_recv()

        by_parity(pos, lambda: go(True), lambda: go(False))

    def finish_shared(gather, pos):
        shared(*gather, pos, True).wait_send()
        shared(*gather, pos, False).wait_send()

    def finish_passed(gather, pos):
        by_parity(pos, lambda: passed(*gather, pos, True).wait_send(), lambda: passed(*gather, pos, False).wait_send())

    x_gather = (x_v, xg_send, xg_recv)
    e_gather = (e_v, eg_send, eg_recv)

    def owner_of(idx):
        return jnp.where(idx < n_chunk, me, far)

    def act_copy(idx):
        dst = x_v.at[lax.rem(idx, n_chunk), owner_of(idx)]
        return remote(yf_v.at[lax.rem(idx, 2)], dst, xp_send.at[idx], xp_recv.at[idx], stage=stage + 1)

    def grad_copy(pos):
        return remote(yb_v.at[lax.rem(pos, 2)], e_v.at[pos, me], ep_send.at[pos], ep_recv.at[pos], stage=stage - 1)

    def forward(idx):
        pos, owner = lax.rem(idx, n_chunk), owner_of(idx)
        kept = jnp.where(idx < n_chunk, pos, n_chunk)

        @pl.when(not_first)
        def _():
            act_copy(idx).wait_recv()
            pl.when(idx < n_chunk)(lambda: start_shared(x_gather, pos))

        @pl.when(not_last & (idx >= 2))
        def _():
            act_copy(idx - 2).wait_send()

        slot = lax.rem(idx, 2)
        for part in range(n_model):
            cols = pl.ds(part * hid, hid)
            pre = dot_nn(x_v[pos, owner], w1_v[part]).astype(jnp.bfloat16)
            u_v[kept, :, cols] = pre
            a_v[:, cols] = gelu_tanh(pre.astype(jnp.float32)).astype(jnp.bfloat16)
        branch = dot_nn(a_v[...], w2_v[...].reshape(n_model * hid, dim))
        yf_v[slot] = (x_v[pos, owner].astype(jnp.float32) + branch).astype(jnp.bfloat16)

        @pl.when(not_last)
        def _():
            act_copy(idx).start()

        @pl.when(is_last)
        def _():
            err = yf_v[slot].astype(jnp.float32) - e_v[pos, me].astype(jnp.float32)
            e_v[pos, me] = (err * grad_scale).astype(jnp.bfloat16)
            loss_acc[...] += jnp.sum((err * err).reshape(-1, 8, dim), axis=0)

    def backward(pos):
        @pl.when(not_last)
        def _():
            grad_copy(pos).wait_recv()

        start_shared(e_gather, pos)

        @pl.when(not_first)
        def _():
            @pl.when(pos >= 2)
            def _():
                grad_copy(pos - 2).wait_send()

            for part in range(n_model):
                cols = pl.ds(part * hid, hid)
                grad_act = dot_nt(e_v[pos, me], w2_v[part]).astype(jnp.bfloat16)
                slope = gelu_slope(u_v[pos, :, cols].astype(jnp.float32))
                a_v[:, cols] = (slope * grad_act.astype(jnp.float32)).astype(jnp.bfloat16)
            branch = dot_nt(a_v[:, pl.ds(0, hid)], w1_v[0])
            for part in range(1, n_model):
                branch += dot_nt(a_v[:, pl.ds(part * hid, hid)], w1_v[part])
            yb_v[lax.rem(pos, 2)] = (e_v[pos, me].astype(jnp.float32) + branch).astype(jnp.bfloat16)
            grad_copy(pos).start()

    def weight_grads(pos):
        @pl.when(not_first)
        def _():
            shared(*x_gather, pos, True).wait_recv()
            shared(*x_gather, pos, False).wait_recv()
            pl.when(is_last)(lambda: act_copy(n_chunk + pos).wait_recv())

        arrived(e_gather, pos)
        pre = dot_nn(x_v[pos].reshape(rows_all, dim), w1_v[me]).astype(jnp.bfloat16)
        du_v[...] = pre
        da_v[...] = gelu_tanh(pre.astype(jnp.float32)).astype(jnp.bfloat16)
        dw2[...] += dot_tn(da_v[...], e_v[pos].reshape(rows_all, dim))
        grad_act = dot_nt(e_v[pos].reshape(rows_all, dim), w2_v[me]).astype(jnp.bfloat16)
        slope = gelu_slope(du_v[...].astype(jnp.float32))
        da_v[...] = (slope * grad_act.astype(jnp.float32)).astype(jnp.bfloat16)
        dw1[...] += dot_tn(x_v[pos].reshape(rows_all, dim), da_v[...])

    def loss_share(kind, peer):
        return remote(loss_parts.at[0], loss_parts.at[1 + kind], loss_send.at[kind], loss_recv.at[kind], model=peer)

    def loss_down():
        return remote(loss_tot, loss_tot, loss_send.at[3], loss_recv.at[3], stage=stage - 1)

    depth = last - stage
    n_forward = jnp.where(is_last, n_chunk, 2 * n_chunk)
    warm = jnp.minimum(2 * n_chunk - 1, depth * (depth + 2))
    is_late = stage >= n_stage // 2
    relay_at = warm + jnp.where(is_late, 5, 1)
    grads_at = warm + jnp.where(is_late, n_chunk, 2)
    loss_at = jnp.where(is_late, grads_at, grads_at + n_chunk - 2)

    def due(turn, start, fn, count=n_chunk):
        pos = turn - start
        pl.when((pos >= 0) & (pos < count))(lambda: fn(pos))

    @pl.loop(0, grads_at + n_chunk)
    def _(turn):
        due(turn, 0, forward, n_forward)
        due(turn, warm, backward)
        due(turn, relay_at, functools.partial(relay, e_gather))

        @pl.when(is_last & (turn == n_chunk - 1))
        def _():
            loss_parts[0] = jnp.full((8, 128), 0.5 * jnp.sum(loss_acc[...]), jnp.float32)

        @pl.when(turn == loss_at)
        def _():
            @pl.when(is_last)
            def _():
                shares = [loss_share(kind, peer) for kind, peer in enumerate((left, right, far))]
                for copy in shares:
                    copy.start()
                for copy in shares:
                    copy.wait()
                pair_sum = (loss_parts[0] + loss_parts[3]) + (loss_parts[1] + loss_parts[2])
                loss_tot[...] = pair_sum * grad_scale

            @pl.when(not_last)
            def _():
                loss_down().wait_recv()

            @pl.when(not_first)
            def _():
                loss_down().start()

        due(turn, grads_at, weight_grads)

    for weight in weights:
        finish_send(*weight)

    @pl.loop(0, n_chunk)
    def _(pos):
        @pl.when(not_first)
        def _():
            finish_shared(x_gather, pos)

        finish_shared(e_gather, pos)
        finish_passed(e_gather, pos)

    for back in (2, 1):
        @pl.when(not_last)
        def _():
            act_copy(2 * n_chunk - back).wait_send()

        @pl.when(not_first)
        def _():
            grad_copy(n_chunk - back).wait_send()

    @pl.when(not_first)
    def _():
        loss_down().wait_send()

    loss_out[...] = loss_tot[...]


def solution(mesh):
    n_stage = mesh.shape["stage"]
    n_model = mesh.shape["model"]

    def stage_step(inputs, targets, w_in, w_out):
        num_micro, num_tokens, dim = inputs.shape
        hid = w_in.shape[3]
        w1, w2 = w_in[0, 0], w_out[0, 0]
        tokens = num_micro * num_tokens
        grad_scale = 1.0 / (tokens * dim)
        n_chunk = tokens // (n_model * CHUNK)
        by_owner = (n_model, n_chunk, CHUNK, dim)
        any_spec = pl.BlockSpec(memory_space=pl.ANY)
        vmem_spec = pl.BlockSpec(memory_space=pltpu.VMEM)
        dma = pltpu.SemaphoreType.DMA
        bf16, f32 = jnp.bfloat16, jnp.float32
        dw1, dw2, loss = pl.pallas_call(
            functools.partial(step_kernel, n_stage, n_model, n_chunk, grad_scale),
            out_shape=(
                jax.ShapeDtypeStruct((dim, hid), f32),
                jax.ShapeDtypeStruct((hid, dim), f32),
                jax.ShapeDtypeStruct((8, 128), f32),
            ),
            in_specs=[any_spec] * 4,
            out_specs=(vmem_spec, vmem_spec, vmem_spec),
            scratch_shapes=[
                pltpu.VMEM((n_model, dim, hid), bf16),
                pltpu.VMEM((n_model, hid, dim), bf16),
                pltpu.VMEM((n_chunk, n_model, CHUNK, dim), bf16),
                pltpu.VMEM((n_chunk, n_model, CHUNK, dim), bf16),
                pltpu.VMEM((2, CHUNK, dim), bf16),
                pltpu.VMEM((2, CHUNK, dim), bf16),
                pltpu.VMEM((n_chunk + 1, CHUNK, n_model * hid), bf16),
                pltpu.VMEM((CHUNK, n_model * hid), bf16),
                pltpu.VMEM((n_model * CHUNK, hid), bf16),
                pltpu.VMEM((n_model * CHUNK, hid), bf16),
                pltpu.VMEM((8, dim), f32),
                pltpu.VMEM((4, 8, 128), f32),
                pltpu.VMEM((8, 128), f32),
                dma((2 + n_model,)), dma((2, 6)), dma((2, 6)),
                dma((2 * n_chunk,)), dma((2 * n_chunk,)), dma((n_chunk,)), dma((n_chunk,)),
                dma((2, n_chunk)), dma((2, n_chunk)), dma((3, n_chunk)), dma((3, n_chunk)),
                dma((4,)), dma((4,)),
            ],
            compiler_params=pltpu.CompilerParams(
                collective_id=0, has_side_effects=True, vmem_limit_bytes=67043328
            ),
        )(inputs.reshape(by_owner), targets.reshape(by_owner), w1, w2)
        return dw1[None, None], dw2[None, None], loss[0, :1]

    return jax.shard_map(
        stage_step,
        mesh=mesh,
        in_specs=(P("data", None, None), P("data", None, None), P("stage", None, None, "model"), P("stage", None, "model", None)),
        out_specs=(P(("data", "stage"), None, None, "model"), P(("data", "stage"), None, "model", None), P("data")),
        check_vma=False,
    )
```

```python
import functools

import jax
import jax.numpy as jnp
from jax import lax
from jax.experimental import pallas as pl
from jax.experimental.pallas import tpu as pltpu
from jax.sharding import PartitionSpec as P

GELU_COEF = 0.7978845608028654
CUBIC_COEF = 0.044715
CHUNK = 128
MESH = pl.DeviceIdType.MESH


def gelu_tanh(values):
    inner_arg = GELU_COEF * (values + CUBIC_COEF * values * values * values)
    return 0.5 * values * (1.0 + jnp.tanh(inner_arg))


def gelu_slope(values):
    square = values * values
    tanh_val = jnp.tanh(GELU_COEF * (values + CUBIC_COEF * values * square))
    return 0.5 * (1.0 + tanh_val) + 0.5 * values * (1.0 - tanh_val * tanh_val) * GELU_COEF * (1.0 + 3.0 * CUBIC_COEF * square)


def dot_nn(lhs, rhs):
    return lax.dot_general(lhs, rhs, (((1,), (0,)), ((), ())), preferred_element_type=jnp.float32)


def dot_nt(lhs, rhs):
    return lax.dot_general(lhs, rhs, (((1,), (1,)), ((), ())), preferred_element_type=jnp.float32)


def dot_tn(lhs, rhs):
    return lax.dot_general(lhs, rhs, (((0,), (0,)), ((), ())), preferred_element_type=jnp.float32)


def step_kernel(
    n_stage, n_model, n_chunk, grad_scale,
    in_hbm, tgt_hbm, w1_hbm, w2_hbm,
    dw1, dw2, loss_out,
    w1_v, w2_v, x_v, e_v, yf_v, yb_v, u_v, a_v, du_v, da_v, loss_acc, loss_parts, loss_tot,
    local_sem, w_send, w_recv,
    xp_send, xp_recv, ep_send, ep_recv,
    xg_send, xg_recv, eg_send, eg_recv,
    loss_send, loss_recv,
):
    stage = lax.axis_index("stage")
    me = lax.axis_index("model")
    last = n_stage - 1
    left = lax.rem(me + n_model - 1, n_model)
    right = lax.rem(me + 1, n_model)
    far = lax.rem(me + 2, n_model)
    is_first = stage == 0
    is_last = stage == last
    not_first = stage > 0
    not_last = stage < last
    dim, hid = w1_v.shape[1], w1_v.shape[2]
    half = dim // 2
    rows_all = n_model * CHUNK

    def remote(src, dst, send, recv, **where):
        return pltpu.make_async_remote_copy(
            src_ref=src, dst_ref=dst, send_sem=send, recv_sem=recv, device_id=where, device_id_type=MESH
        )

    barrier = pltpu.get_barrier_semaphore()
    for peer in (left, right, far):
        pl.semaphore_signal(barrier, inc=1, device_id={"model": peer}, device_id_type=MESH)

    @pl.when(not_first)
    def _():
        pl.semaphore_signal(barrier, inc=1, device_id={"stage": stage - 1}, device_id_type=MESH)

    @pl.when(not_last)
    def _():
        pl.semaphore_signal(barrier, inc=1, device_id={"stage": stage + 1}, device_id_type=MESH)

    num_peers = 5 - is_first.astype(jnp.int32) - is_last.astype(jnp.int32)
    pl.semaphore_wait(barrier, num_peers)

    def own_piece(w_hbm, w_v, idx, part, peer, slot):
        rows = pl.ds(part * half, half)
        return remote(w_hbm.at[rows], w_v.at[me, rows], w_send.at[idx, slot], w_recv.at[idx, slot], model=peer)

    def passed_piece(w_v, idx, owner, part, peer, slot):
        rows = pl.ds(part * half, half)
        return remote(w_v.at[owner, rows], w_v.at[owner, rows], w_send.at[idx, slot], w_recv.at[idx, slot], model=peer)

    weights = ((w1_hbm, w1_v, 0), (w2_hbm, w2_v, 1))
    def start_own(w_hbm, w_v, idx):
        own_piece(w_hbm, w_v, idx, 0, right, 0).start()
        own_piece(w_hbm, w_v, idx, 1, left, 3).start()
        own_piece(w_hbm, w_v, idx, 1, right, 1).start()
        own_piece(w_hbm, w_v, idx, 0, left, 2).start()

    def pass_on(w_hbm, w_v, idx):
        own_piece(w_hbm, w_v, idx, 0, right, 0).wait_recv()
        passed_piece(w_v, idx, left, 0, right, 4).start()
        own_piece(w_hbm, w_v, idx, 1, left, 3).wait_recv()
        passed_piece(w_v, idx, right, 1, left, 5).start()

    def finish_recv(w_hbm, w_v, idx):
        own_piece(w_hbm, w_v, idx, 1, right, 1).wait_recv()
        own_piece(w_hbm, w_v, idx, 0, left, 2).wait_recv()
        passed_piece(w_v, idx, left, 0, right, 4).wait_recv()
        passed_piece(w_v, idx, right, 1, left, 5).wait_recv()

    def finish_send(w_hbm, w_v, idx):
        own_piece(w_hbm, w_v, idx, 0, right, 0).wait_send()
        own_piece(w_hbm, w_v, idx, 1, left, 3).wait_send()
        own_piece(w_hbm, w_v, idx, 1, right, 1).wait_send()
        own_piece(w_hbm, w_v, idx, 0, left, 2).wait_send()
        passed_piece(w_v, idx, left, 0, right, 4).wait_send()
        passed_piece(w_v, idx, right, 1, left, 5).wait_send()

    start_own(*weights[0])
    own_copies = [pltpu.make_async_copy(w_hbm, w_v.at[me], local_sem.at[idx]) for w_hbm, w_v, idx in weights]
    for copy in own_copies:
        copy.start()

    @pl.when(is_first)
    def _():
        loads = [pltpu.make_async_copy(in_hbm.at[owner], x_v.at[:, owner], local_sem.at[2 + owner]) for owner in range(n_model)]
        for load in loads:
            load.start()
        for load in loads:
            load.wait()

    @pl.when(is_last)
    def _():
        load = pltpu.make_async_copy(tgt_hbm.at[me], e_v.at[:, me], local_sem.at[2])
        load.start()
        load.wait()
        loss_acc[...] = jnp.zeros_like(loss_acc)

    dw1[...] = jnp.zeros_like(dw1)
    dw2[...] = jnp.zeros_like(dw2)

    pass_on(*weights[0])
    start_own(*weights[1])
    pass_on(*weights[1])
    for copy in own_copies:
        copy.wait()
    finish_recv(*weights[0])
    finish_recv(*weights[1])

    def shared(buf, send, recv, pos, to_right):
        kind, peer = (0, right) if to_right else (1, left)
        return remote(buf.at[pos, me], buf.at[pos, me], send.at[kind, pos], recv.at[kind, pos], model=peer)

    def passed(buf, send, recv, pos, to_right):
        owner, peer = (left, right) if to_right else (right, left)
        return remote(buf.at[pos, owner], buf.at[pos, owner], send.at[2, pos], recv.at[2, pos], model=peer)

    def start_shared(gather, pos):
        shared(*gather, pos, True).start()
        shared(*gather, pos, False).start()

    def by_parity(pos, even_fn, odd_fn):
        pl.when(lax.rem(pos, 2) == 0)(even_fn)
        pl.when(lax.rem(pos, 2) == 1)(odd_fn)

    def relay(gather, pos):
        def go(to_right):
            shared(*gather, pos, to_right).wait_recv()
            passed(*gather, pos, to_right).start()

        by_parity(pos, lambda: go(True), lambda: go(False))

    def arrived(gather, pos):
        def go(to_right):
            shared(*gather, pos, not to_right).wait_recv()
            passed(*gather, pos, to_right).wait_recv()

        by_parity(pos, lambda: go(True), lambda: go(False))

    def finish_shared(gather, pos):
        shared(*gather, pos, True).wait_send()
        shared(*gather, pos, False).wait_send()

    def finish_passed(gather, pos):
        by_parity(pos, lambda: passed(*gather, pos, True).wait_send(), lambda: passed(*gather, pos, False).wait_send())

    x_gather = (x_v, xg_send, xg_recv)
    e_gather = (e_v, eg_send, eg_recv)

    def owner_of(idx):
        return jnp.where(idx < n_chunk, me, far)

    def act_copy(idx):
        dst = x_v.at[lax.rem(idx, n_chunk), owner_of(idx)]
        return remote(yf_v.at[lax.rem(idx, 2)], dst, xp_send.at[idx], xp_recv.at[idx], stage=stage + 1)

    def grad_copy(pos):
        return remote(yb_v.at[lax.rem(pos, 2)], e_v.at[pos, me], ep_send.at[pos], ep_recv.at[pos], stage=stage - 1)

    def forward(idx):
        pos, owner = lax.rem(idx, n_chunk), owner_of(idx)
        kept = jnp.where(idx < n_chunk, pos, n_chunk)

        @pl.when(not_first)
        def _():
            act_copy(idx).wait_recv()
            pl.when(idx < n_chunk)(lambda: start_shared(x_gather, pos))

        @pl.when(not_last & (idx >= 2))
        def _():
            act_copy(idx - 2).wait_send()

        slot = lax.rem(idx, 2)
        for part in range(n_model):
            cols = pl.ds(part * hid, hid)
            pre = dot_nn(x_v[pos, owner], w1_v[part]).astype(jnp.bfloat16)
            u_v[kept, :, cols] = pre
            a_v[:, cols] = gelu_tanh(pre.astype(jnp.float32)).astype(jnp.bfloat16)
        branch = dot_nn(a_v[...], w2_v[...].reshape(n_model * hid, dim))
        yf_v[slot] = (x_v[pos, owner].astype(jnp.float32) + branch).astype(jnp.bfloat16)

        @pl.when(not_last)
        def _():
            act_copy(idx).start()

        @pl.when(is_last)
        def _():
            err = yf_v[slot].astype(jnp.float32) - e_v[pos, me].astype(jnp.float32)
            e_v[pos, me] = (err * grad_scale).astype(jnp.bfloat16)
            loss_acc[...] += jnp.sum((err * err).reshape(-1, 8, dim), axis=0)

    def backward(pos):
        @pl.when(not_last)
        def _():
            grad_copy(pos).wait_recv()

        start_shared(e_gather, pos)

        @pl.when(not_first)
        def _():
            @pl.when(pos >= 2)
            def _():
                grad_copy(pos - 2).wait_send()

            for part in range(n_model):
                cols = pl.ds(part * hid, hid)
                grad_act = dot_nt(e_v[pos, me], w2_v[part]).astype(jnp.bfloat16)
                slope = gelu_slope(u_v[pos, :, cols].astype(jnp.float32))
                a_v[:, cols] = (slope * grad_act.astype(jnp.float32)).astype(jnp.bfloat16)
            branch = dot_nt(a_v[:, pl.ds(0, hid)], w1_v[0])
            for part in range(1, n_model):
                branch += dot_nt(a_v[:, pl.ds(part * hid, hid)], w1_v[part])
            yb_v[lax.rem(pos, 2)] = (e_v[pos, me].astype(jnp.float32) + branch).astype(jnp.bfloat16)
            grad_copy(pos).start()

    def weight_grads(pos):
        @pl.when(not_first)
        def _():
            shared(*x_gather, pos, True).wait_recv()
            shared(*x_gather, pos, False).wait_recv()
            pl.when(is_last)(lambda: act_copy(n_chunk + pos).wait_recv())

        arrived(e_gather, pos)
        pre = dot_nn(x_v[pos].reshape(rows_all, dim), w1_v[me]).astype(jnp.bfloat16)
        du_v[...] = pre
        da_v[...] = gelu_tanh(pre.astype(jnp.float32)).astype(jnp.bfloat16)
        dw2[...] += dot_tn(da_v[...], e_v[pos].reshape(rows_all, dim))
        grad_act = dot_nt(e_v[pos].reshape(rows_all, dim), w2_v[me]).astype(jnp.bfloat16)
        slope = gelu_slope(du_v[...].astype(jnp.float32))
        da_v[...] = (slope * grad_act.astype(jnp.float32)).astype(jnp.bfloat16)
        dw1[...] += dot_tn(x_v[pos].reshape(rows_all, dim), da_v[...])

    def loss_share(kind, peer):
        return remote(loss_parts.at[0], loss_parts.at[1 + kind], loss_send.at[kind], loss_recv.at[kind], model=peer)

    def loss_down():
        return remote(loss_tot, loss_tot, loss_send.at[3], loss_recv.at[3], stage=stage - 1)

    depth = last - stage
    n_forward = jnp.where(is_last, n_chunk, 2 * n_chunk)
    warm = jnp.minimum(2 * n_chunk - 1, depth * (depth + 2))
    is_late = stage >= n_stage // 2
    relay_at = warm + jnp.where(is_late, 5, 1)
    grads_at = warm + jnp.where(is_late, n_chunk, 2)
    loss_at = jnp.where(is_late, grads_at, grads_at + n_chunk - 2)

    def due(turn, start, fn, count=n_chunk):
        pos = turn - start
        pl.when((pos >= 0) & (pos < count))(lambda: fn(pos))

    @pl.loop(0, grads_at + n_chunk)
    def _(turn):
        due(turn, 0, forward, n_forward)
        due(turn, warm, backward)
        due(turn, relay_at, functools.partial(relay, e_gather))

        @pl.when(is_last & (turn == n_chunk - 1))
        def _():
            loss_parts[0] = jnp.full((8, 128), 0.5 * jnp.sum(loss_acc[...]), jnp.float32)

        @pl.when(turn == loss_at)
        def _():
            @pl.when(is_last)
            def _():
                shares = [loss_share(kind, peer) for kind, peer in enumerate((left, right, far))]
                for copy in shares:
                    copy.start()
                for copy in shares:
                    copy.wait()
                pair_sum = (loss_parts[0] + loss_parts[3]) + (loss_parts[1] + loss_parts[2])
                loss_tot[...] = pair_sum * grad_scale

            @pl.when(not_last)
            def _():
                loss_down().wait_recv()

            @pl.when(not_first)
            def _():
                loss_down().start()

        due(turn, grads_at, weight_grads)

    for weight in weights:
        finish_send(*weight)

    @pl.loop(0, n_chunk)
    def _(pos):
        @pl.when(not_first)
        def _():
            finish_shared(x_gather, pos)

        finish_shared(e_gather, pos)
        finish_passed(e_gather, pos)

    for back in (2, 1):
        @pl.when(not_last)
        def _():
            act_copy(2 * n_chunk - back).wait_send()

        @pl.when(not_first)
        def _():
            grad_copy(n_chunk - back).wait_send()

    @pl.when(not_first)
    def _():
        loss_down().wait_send()

    loss_out[...] = loss_tot[...]


def solution(mesh):
    n_stage = mesh.shape["stage"]
    n_model = mesh.shape["model"]

    def stage_step(inputs, targets, w_in, w_out):
        num_micro, num_tokens, dim = inputs.shape
        hid = w_in.shape[3]
        w1, w2 = w_in[0, 0], w_out[0, 0]
        tokens = num_micro * num_tokens
        grad_scale = 1.0 / (tokens * dim)
        n_chunk = tokens // (n_model * CHUNK)
        by_owner = (n_model, n_chunk, CHUNK, dim)
        any_spec = pl.BlockSpec(memory_space=pl.ANY)
        vmem_spec = pl.BlockSpec(memory_space=pltpu.VMEM)
        dma = pltpu.SemaphoreType.DMA
        bf16, f32 = jnp.bfloat16, jnp.float32
        dw1, dw2, loss = pl.pallas_call(
            functools.partial(step_kernel, n_stage, n_model, n_chunk, grad_scale),
            out_shape=(
                pltpu.VMEM((dim, hid), f32),
                pltpu.VMEM((hid, dim), f32),
                jax.ShapeDtypeStruct((8, 128), f32),
            ),
            in_specs=[any_spec] * 4,
            out_specs=(vmem_spec, vmem_spec, vmem_spec),
            scratch_shapes=[
                pltpu.VMEM((n_model, dim, hid), bf16),
                pltpu.VMEM((n_model, hid, dim), bf16),
                pltpu.VMEM((n_chunk, n_model, CHUNK, dim), bf16),
                pltpu.VMEM((n_chunk, n_model, CHUNK, dim), bf16),
                pltpu.VMEM((2, CHUNK, dim), bf16),
                pltpu.VMEM((2, CHUNK, dim), bf16),
                pltpu.VMEM((n_chunk + 1, CHUNK, n_model * hid), bf16),
                pltpu.VMEM((CHUNK, n_model * hid), bf16),
                pltpu.VMEM((n_model * CHUNK, hid), bf16),
                pltpu.VMEM((n_model * CHUNK, hid), bf16),
                pltpu.VMEM((8, dim), f32),
                pltpu.VMEM((4, 8, 128), f32),
                pltpu.VMEM((8, 128), f32),
                dma((2 + n_model,)), dma((2, 6)), dma((2, 6)),
                dma((2 * n_chunk,)), dma((2 * n_chunk,)), dma((n_chunk,)), dma((n_chunk,)),
                dma((2, n_chunk)), dma((2, n_chunk)), dma((3, n_chunk)), dma((3, n_chunk)),
                dma((4,)), dma((4,)),
            ],
            compiler_params=pltpu.CompilerParams(
                collective_id=0, has_side_effects=True, vmem_limit_bytes=58000000
            ),
        )(inputs.reshape(by_owner), targets.reshape(by_owner), w1, w2)
        return dw1[None, None], dw2[None, None], loss[0, :1]

    return jax.shard_map(
        stage_step,
        mesh=mesh,
        in_specs=(P("data", None, None), P("data", None, None), P("stage", None, None, "model"), P("stage", None, "model", None)),
        out_specs=(P(("data", "stage"), None, None, "model"), P(("data", "stage"), None, "model", None), P("data")),
        check_vma=False,
    )
```
